32 devices in a mesh: groups: 2 (over x), kvseq: 8 (over z, y), tensor: 2 (over core).
Axes of the slice: x: 2, y: 2, z: 4, core: 2. Of those that a mesh axis runs over, the one named last changes fastest.
Arguments:
- hidden: bfloat16 [16, 8192], P('groups', 'kvseq'), parts along dimension 0, may hold values from -30 to 30
- lengths: int32 [16], P('groups'), parts along dimension 0, may hold values from 128 to 2048, as said below
- key_cache: bfloat16 [16, 2048, 1024], P('groups', 'kvseq', 'tensor'), parts along dimension 0, may hold values from -400 to 400
- value_cache: bfloat16 [16, 2048, 1024], P('groups', 'kvseq', 'tensor'), parts along dimension 0, may hold values from -60 to 60
- gain_in: float32 [8192], P('kvseq'), may hold values from 0.1 to 1.9
- w_query: bfloat16 [8192, 8192], P('kvseq', 'tensor'), may hold values from -0.0625 to 0.0625
- w_key: bfloat16 [8192, 1024], P('kvseq', 'tensor'), may hold values from -0.0625 to 0.0625
- w_value: bfloat16 [8192, 1024], P('kvseq', 'tensor'), may hold values from -0.0625 to 0.0625
- w_output: bfloat16 [8192, 8192], P('tensor', 'kvseq'), may hold values from -0.0625 to 0.0625
- gain_post: float32 [8192], P('kvseq'), may hold values from 0.1 to 1.9
- w_gate: bfloat16 [8192, 15360], P('kvseq', 'tensor'), may hold values from -0.0625 to 0.0625
- w_up: bfloat16 [8192, 15360], P('kvseq', 'tensor'), may hold values from -0.0625 to 0.0625
- w_down: bfloat16 [15360, 8192], P('tensor', 'kvseq'), may hold values from -0.046875 to 0.046875
Outputs:
- output: bfloat16 [16, 8192], P('groups', 'kvseq'), parts along dimension 0
- new_keys: bfloat16 [16, 1024], P('groups', 'tensor'), parts along dimension 0
- new_values: bfloat16 [16, 1024], P('groups', 'tensor'), parts along dimension 0
The draws below stay inside these ranges and needn't reach their ends.
There are 2 independent parts, one for each index of `groups`. The reference program is written for one: setup_inputs(seed, part) draws one part's arguments, and reference() takes and returns one part's arrays. A program takes and returns all parts, laid end to end along the dimension named above; an argument that names none is the same for every part. Nothing has to cross between parts.
Inputs may be any that keep to these rules, and one draw needn't show every extreme that they name: `lengths`: multiples of 128; some sequence holds exactly 2048.
All inputs are finite; a program needn't handle non-finite values.
Results may differ from the reference program's by a relative error of at most 0.024.
Values may be sent and summed in bfloat16 or wider, within the bound.
A program may use at most 128 MiB of HBM per device.

```python
import jax
import jax.numpy as jnp
from jax import lax

D = 8192
H = 64
KVH = 8
HD = 128
FF = 15360
SEQS = 8
PAGE = 128
LENGTH = 2048


def draw_hidden(key, part):
    ramp = jnp.exp(jnp.linspace(0.0, jnp.log(3.0), D)).astype(jnp.float32)
    rough = jax.random.uniform(jax.random.fold_in(key, 11), (D,), jnp.float32, 0.5, 1.5)
    base = jnp.clip(jax.random.normal(jax.random.fold_in(key, 12), (SEQS, D), jnp.float32), -6.0, 6.0)
    return (base * ramp * rough).astype(jnp.bfloat16)


def draw_lengths(key, part):
    pages = jax.random.randint(jax.random.fold_in(key, 21), (SEQS,), 1, LENGTH // PAGE + 1) * PAGE
    chosen = jax.random.randint(jax.random.fold_in(key, 22), (), 0, SEQS)
    return pages.at[chosen].set(LENGTH).astype(jnp.int32)


def draw_key_cache(key, part):
    base = jnp.clip(jax.random.normal(jax.random.fold_in(key, 31), (SEQS, LENGTH, KVH * HD), jnp.float32), -6.0, 6.0)
    return base.astype(jnp.bfloat16)


def draw_value_cache(key, part):
    place = jnp.arange(LENGTH, dtype=jnp.float32) / LENGTH
    magnitude = jax.random.uniform(jax.random.fold_in(key, 41), (KVH * HD,), jnp.float32, 0.5, 1.5)
    sign = jnp.where(jax.random.bernoulli(jax.random.fold_in(key, 42), 0.5, (KVH * HD,)), 1.0, -1.0)
    common = 1.5 * magnitude * sign
    ramp = jnp.exp(place * jnp.log(4.0))
    rough = jnp.clip(jax.random.normal(jax.random.fold_in(key, 43), (SEQS, LENGTH, KVH * HD), jnp.float32), -3.0, 3.0)
    values = (rough + common[None, None, :]) * ramp[None, :, None]
    return values.astype(jnp.bfloat16)


def shard_levels(rng, extent, shards, least, high):
    level = 1.0
    for dim, parts in shards:
        draws = jax.random.uniform(jax.random.fold_in(jax.random.fold_in(rng, 6), dim), (parts,), jnp.float32, least / len(shards), high / len(shards))
        level = level * jnp.repeat(jnp.exp(draws), extent[dim] // parts).reshape((-1,) + (1,) * (len(extent) - 1 - dim))
    return level


def bell_draw(rng, shape, spread, limit, split=(), kind=jnp.bfloat16):
    drawn = spread * jax.random.normal(rng, shape, jnp.float32)
    if split:
        drawn = drawn * shard_levels(rng, shape, split, -0.22, 0.18)
    return jnp.clip(drawn, -limit, limit).astype(kind)


def setup_inputs(seed: int = 0, part: int = 0) -> dict:
    key_list = jax.random.split(jax.random.key(seed), 14)
    part_splits = jax.random.split(jax.random.fold_in(key_list[13], part), 14)
    hidden = draw_hidden(jax.random.fold_in(jax.random.fold_in(key_list[13], part), 71), part)
    lengths = draw_lengths(jax.random.fold_in(jax.random.fold_in(key_list[13], part), 71), part)
    key_cache = draw_key_cache(jax.random.fold_in(jax.random.fold_in(key_list[13], part), 71), part)
    value_cache = draw_value_cache(jax.random.fold_in(jax.random.fold_in(key_list[13], part), 71), part)
    gain_in = jnp.clip(1.0 + 0.18 * jax.random.normal(key_list[4], (D,), jnp.float32), 0.1, 1.9)
    w_query = bell_draw(key_list[5], (D, H * HD), D ** -0.5, 0.0625, ((0, 8), (1, 2)))
    w_key = bell_draw(key_list[6], (D, KVH * HD), D ** -0.5, 0.0625, ((0, 8), (1, 2)))
    w_value = bell_draw(key_list[7], (D, KVH * HD), D ** -0.5, 0.0625, ((0, 8), (1, 2)))
    w_output = bell_draw(key_list[8], (H * HD, D), (H * HD) ** -0.5, 0.0625, ((0, 2), (1, 8)))
    gain_post = jnp.clip(1.0 + 0.18 * jax.random.normal(key_list[9], (D,), jnp.float32), 0.1, 1.9)
    w_gate = bell_draw(key_list[10], (D, FF), D ** -0.5, 0.0625, ((0, 8), (1, 2)))
    w_up = bell_draw(key_list[11], (D, FF), D ** -0.5, 0.0625, ((0, 8), (1, 2)))
    w_down = bell_draw(key_list[12], (FF, D), FF ** -0.5, 0.046875, ((0, 2), (1, 8)))
    return dict(hidden=hidden, lengths=lengths, key_cache=key_cache, value_cache=value_cache, gain_in=gain_in, w_query=w_query, w_key=w_key, w_value=w_value, w_output=w_output, gain_post=gain_post, w_gate=w_gate, w_up=w_up, w_down=w_down)


epsilon = 1e-06
rope_base = 1000000.0

def rotate(values, position):
    half_dim = values.shape[-1] // 2
    frequency = rope_base ** (-jnp.arange(half_dim, dtype=jnp.float32) * 2.0 / values.shape[-1])
    angles = position[:, None, None] * frequency
    cosine = jnp.cos(angles)
    sine = jnp.sin(angles)
    lower = values[..., :half_dim]
    upper = values[..., half_dim:]
    return jnp.concatenate([lower * cosine - upper * sine, upper * cosine + lower * sine], axis=-1)

def rms_norm(stream, gain):
    scale = lax.rsqrt(lax.optimization_barrier(jnp.mean(stream * stream, axis=1, keepdims=True)) + epsilon)
    return (stream * scale * gain).astype(jnp.bfloat16)

def reference(hidden, lengths, key_cache, value_cache, gain_in, w_query, w_key, w_value, w_output, gain_post, w_gate, w_up, w_down):
    stream = hidden.astype(jnp.float32)
    normed = rms_norm(stream, gain_in)
    query = jnp.dot(normed, w_query, preferred_element_type=jnp.float32)
    key = jnp.dot(normed, w_key, preferred_element_type=jnp.float32)
    value = jnp.dot(normed, w_value, preferred_element_type=jnp.float32)
    position = lengths.astype(jnp.float32)
    query = rotate(query.reshape(SEQS, H, HD), position)
    new_keys = rotate(key.reshape(SEQS, KVH, HD), position).astype(jnp.bfloat16)
    new_values = value.reshape(SEQS, KVH, HD).astype(jnp.bfloat16)
    grouped = query.astype(jnp.bfloat16).reshape(SEQS, KVH, H // KVH, HD).astype(jnp.float32)
    cached_keys = key_cache.reshape(SEQS, LENGTH, KVH, HD).astype(jnp.float32)
    cached_values = value_cache.reshape(SEQS, LENGTH, KVH, HD).astype(jnp.float32)
    factor = float(HD) ** (-0.5)
    scores = jnp.einsum('skgd,slkd->skgl', grouped, cached_keys) * factor
    valid = (jnp.arange(LENGTH, dtype=jnp.int32)[None, :] < lengths[:, None])[:, None, None, :]
    masked = jnp.where(valid, scores, -1e+30)
    own = jnp.einsum('skgd,skd->skg', grouped, new_keys.astype(jnp.float32)) * factor
    top = jnp.maximum(lax.optimization_barrier(jnp.max(masked, axis=-1)), own)
    weights = jnp.where(valid, jnp.exp(masked - top[..., None]), 0.0)
    own_weight = jnp.exp(own - top)
    total = lax.optimization_barrier(jnp.sum(weights, axis=-1)) + own_weight
    mixed = jnp.einsum('skgl,slkd->skgd', weights.astype(jnp.bfloat16).astype(jnp.float32), cached_values)
    mixed = mixed + own_weight[..., None] * new_values.astype(jnp.float32)[:, :, None, :]
    attended = (mixed / total[..., None]).astype(jnp.bfloat16).reshape(SEQS, H * HD)
    residual = stream + jnp.dot(attended, w_output, preferred_element_type=jnp.float32)
    normed_post = rms_norm(residual, gain_post)
    gate = jnp.dot(normed_post, w_gate, preferred_element_type=jnp.float32)
    upward = jnp.dot(normed_post, w_up, preferred_element_type=jnp.float32)
    inner = (jax.nn.silu(gate) * upward).astype(jnp.bfloat16)
    output = (residual + jnp.dot(inner, w_down, preferred_element_type=jnp.float32)).astype(jnp.bfloat16)
    return (output, new_keys.reshape(SEQS, KVH * HD), new_values.reshape(SEQS, KVH * HD))
```

```python
import functools

import jax
import jax.numpy as jnp
import numpy as np
from jax import lax
from jax.experimental import pallas as pl
from jax.experimental.pallas import tpu as pltpu
from jax.sharding import PartitionSpec as P

HD = 128
epsilon = 1e-06
rope_base = 1000000.0
BF = jnp.bfloat16
F32 = jnp.float32
MESH = pl.DeviceIdType.MESH


def mult(x, m):
    return pl.multiple_of(x, m)


def when(cond, f):
    if cond is True:
        f()
    else:
        pl.when(cond)(f)


def layer_kernel(
    c,
    lengths,
    hidden,
    gain_in,
    gain_post,
    freq,
    kc_hbm,
    vc_hbm,
    wq_hbm,
    wk_hbm,
    wv_hbm,
    wo_hbm,
    wg_hbm,
    wu_hbm,
    wd_hbm,
    out,
    new_keys,
    new_values,
    wqkv,
    tail,
    wo,
    wg,
    wu,
    kc,
    vc,
    send_a,
    recv_a,
    all_a,
    send_b,
    recv_b,
    send_m,
    recv_m,
    all_b,
    part_1,
    send_c,
    recv_c,
    all_c,
    part_2,
    wsem,
    dsem,
    sa_s,
    sa_r,
    ga_s,
    ga_r,
    sb_s,
    sb_r,
    sm_s,
    sm_r,
    gb_s,
    gb_r,
    t1_s,
    t1_r,
    sc_s,
    sc_r,
    gc_s,
    gc_r,
    t2_s,
    t2_r,
):
    n, T, A = c["n"], c["T"], c["A"]
    S, Dl, L = c["S"], c["Dl"], c["L"]
    QH, KH, W = c["QH"], c["KH"], c["W"]
    QC, KC = QH * HD, KH * HD
    TOT = QC + 2 * KC
    CA = TOT // A
    HA = CA // HD
    HB = QH // A
    CB = HB * HD
    FT = c["FT"]
    reuse = c["reuse"]
    per_group = QH // KH
    D = float(Dl * n)
    me = lax.axis_index("kvseq")
    t = lax.axis_index("tensor")
    owner = True if n == A else me < A

    def local(src, dst, sem):
        return pltpu.make_async_copy(src, dst, sem)

    first = [
        local(wq_hbm, wqkv.at[:, pl.ds(0, QC)], wsem.at[0]),
        local(wk_hbm, wqkv.at[:, pl.ds(QC, KC)], wsem.at[1]),
        local(wv_hbm, wqkv.at[:, pl.ds(QC + KC, KC)], wsem.at[2]),
    ]
    later = [
        local(kc_hbm, kc, wsem.at[3]),
        local(vc_hbm, vc, wsem.at[4]),
        local(wo_hbm, wo, wsem.at[5]),
        local(wg_hbm, wg, wsem.at[6]),
        local(wu_hbm, wu, wsem.at[7]),
    ]

    def down_slot(d):
        return wqkv.at[:, pl.ds(d * Dl, Dl)] if d < reuse else tail.at[d - reuse]

    down = [
        local(wd_hbm.at[pl.ds((d * FT // A) * HD, W), :], down_slot(d), dsem.at[d])
        for d in range(A)
    ]
    for x in first:
        x.start()

    barrier = pltpu.get_barrier_semaphore()

    def greet(k, _):
        pl.semaphore_signal(
            barrier, inc=1, device_id={"kvseq": lax.rem(me + k, n)}, device_id_type=MESH
        )
        return 0

    lax.fori_loop(1, n, greet, 0)
    for k in range(1, T):
        pl.semaphore_signal(
            barrier, inc=1, device_id={"tensor": lax.rem(t + k, T)}, device_id_type=MESH
        )

    def remote(src, dst, s_sem, r_sem, to):
        return pltpu.make_async_remote_copy(
            src_ref=src, dst_ref=dst, send_sem=s_sem, recv_sem=r_sem, device_id=to,
            device_id_type=MESH,
        )

    def scatter(send, recv, s_sem, r_sem, d):
        return remote(send.at[d], recv.at[me], s_sem.at[d], r_sem.at[me], {"kvseq": d})

    def scatter_wait_recv(send, recv, s_sem, r_sem):
        def one(k, _):
            src = lax.rem(me + k, n)
            remote(
                send.at[0], recv.at[src], s_sem.at[0], r_sem.at[src], {"kvseq": src}
            ).wait_recv()
            return 0

        lax.fori_loop(1, n, one, 0)

    def scatter_wait_send(send, recv, s_sem, r_sem):
        for d in range(A):
            pl.when(d != me)(lambda d=d: scatter(send, recv, s_sem, r_sem, d).wait_send())

    def gather_start(view, s_sem, r_sem):
        def one(k, _):
            to = lax.rem(me + k, n)
            remote(view(me), view(me), s_sem.at[k], r_sem.at[me], {"kvseq": to}).start()
            return 0

        lax.fori_loop(1, n, one, 0)

    def gather_wait_recv(view, s_sem, r_sem):
        def one(s, _):
            @pl.when(s != me)
            def _():
                remote(view(s), view(s), s_sem.at[0], r_sem.at[s], {"kvseq": s}).wait_recv()

            return 0

        lax.fori_loop(0, A, one, 0)

    def gather_wait_send(view, s_sem, r_sem):
        def one(k, _):
            to = lax.rem(me + k, n)
            remote(view(me), view(me), s_sem.at[k], r_sem.at[me], {"kvseq": to}).wait_send()
            return 0

        def run():
            lax.fori_loop(1, n, one, 0)

        when(owner, run)

    def pair_copies(part, s_sem, r_sem):
        return [
            remote(
                part.at[t], part.at[t], s_sem.at[k], r_sem.at[t], {"tensor": lax.rem(t + k, T)}
            )
            for k in range(1, T)
        ]

    def pair_sum(part, s_sem, r_sem):
        for x in pair_copies(part, s_sem, r_sem):
            x.start()
        for k in range(1, T):
            src = lax.rem(t + k, T)
            remote(
                part.at[src], part.at[src], s_sem.at[k], r_sem.at[src], {"tensor": src}
            ).wait_recv()
        total = part[0]
        for i in range(1, T):
            total = total + part[i]
        return total

    lane = lax.broadcasted_iota(jnp.int32, (S, HD), 1)
    row = lax.broadcasted_iota(jnp.int32, (S, HD), 0)

    def squares_block(x):
        s = jnp.broadcast_to(jnp.sum(x * x, axis=1, keepdims=True), (S, HD))
        high = s.astype(BF).astype(F32)
        return jnp.where(lane < HD // 2, high, s - high).astype(BF)

    def row_scale(block):
        total = jnp.sum(block, axis=1, keepdims=True) * (2.0 / HD)
        return lax.rsqrt(total / D + epsilon)

    stream = hidden[...].astype(F32)
    xg = (stream * gain_in[...]).astype(BF)
    sq = squares_block(stream)

    position = jnp.zeros((S, HD), F32)
    for s in range(S):
        position = jnp.where(row == s, lengths[s].astype(F32), position)
    angle = position * freq[...]
    cosine = jnp.cos(angle)
    sine = jnp.sin(angle)
    sine = jnp.where(lane < HD // 2, -sine, sine)

    for x in first:
        x.wait()
    for x in later + down[reuse:]:
        x.start()
    pl.semaphore_wait(barrier, (n - 1) + (T - 1))

    def project(k, _):
        d = lax.rem(me + 1 + k, A)
        part = jnp.dot(xg, wqkv[:, pl.ds(mult(d * CA, HD), CA)], preferred_element_type=F32)
        send_a[d, :, :CA] = part.astype(BF)
        send_a[d, :, CA:] = sq

        @pl.when(d != me)
        def _():
            scatter(send_a, recv_a, sa_s, sa_r, d).start()

        return 0

    lax.fori_loop(0, A, project, 0)
    for x in down[:reuse]:
        x.start()

    def view_a(s):
        return all_a.at[:, pl.ds(mult(s * CA, HD), CA)]

    def reduce_a():
        recv_a[me] = send_a[me]
        scatter_wait_recv(send_a, recv_a, sa_s, sa_r)
        total = lax.fori_loop(
            1, n, lambda s, acc: acc + recv_a[s].astype(F32), recv_a[0].astype(F32)
        )
        scale = row_scale(total[:, CA:])
        for j in range(HA):
            v = total[:, j * HD : (j + 1) * HD] * scale
            turned = v * cosine + pltpu.roll(v, HD // 2, 1) * sine
            rot = jnp.broadcast_to(me * HA + j, (S, HD)) < QH + KH
            res = jnp.where(rot, turned, v).astype(BF)
            all_a[:, pl.ds(mult((me * HA + j) * HD, HD), HD)] = res
        gather_start(view_a, ga_s, ga_r)

    when(owner, reduce_a)
    gather_wait_recv(view_a, ga_s, ga_r)
    new_keys[...] = all_a[:, QC : QC + KC]
    new_values[...] = all_a[:, QC + KC :]

    R = per_group * S
    brow = lax.broadcasted_iota(jnp.int32, (R, L), 0) % S
    orow = lax.broadcasted_iota(jnp.int32, (R, HD), 0) % S
    limit = jnp.zeros((R, L), jnp.int32)
    for s in range(S):
        limit = jnp.where(brow == s, lengths[s], limit)
    place = lax.broadcasted_iota(jnp.int32, (R, L), 1) + me * L
    valid = place < limit
    factor = float(HD) ** (-0.5)
    later[0].wait()
    later[1].wait()

    def attend(g, _):
        q = jnp.concatenate(
            [
                all_a[:, pl.ds(mult((g * per_group + j) * HD, HD), HD)].astype(F32)
                for j in range(per_group)
            ],
            axis=0,
        ).astype(BF)
        scores = jnp.zeros((R, L), F32)
        for s in range(S):
            keys = kc[s, :, pl.ds(mult(g * HD, HD), HD)]
            x = lax.dot_general(
                q, keys, (((1,), (1,)), ((), ())), preferred_element_type=F32
            )
            scores = jnp.where(brow == s, x, scores)
        scores = jnp.where(valid, scores * factor, -1e30)
        top = jnp.max(scores, axis=1, keepdims=True)
        w = jnp.where(valid, jnp.exp(scores - top), 0.0)
        total = jnp.sum(w, axis=1, keepdims=True)
        w = w.astype(BF)
        mixed = jnp.zeros((R, HD), F32)
        for s in range(S):
            vals = vc[s, :, pl.ds(mult(g * HD, HD), HD)]
            x = jnp.dot(w, vals, preferred_element_type=F32)
            mixed = jnp.where(orow == s, x, mixed)
        for i in range(per_group // HB):
            d = g * (per_group // HB) + i
            ml = jnp.zeros((S, HD), F32)
            for j in range(HB):
                r = (i * HB + j) * S
                send_b[d, :, j * HD : (j + 1) * HD] = mixed[r : r + S].astype(BF)
                ml = jnp.where(lane == j, top[r : r + S], ml)
                ml = jnp.where(lane == HD // 2 + j, total[r : r + S], ml)
            send_m[d] = ml

            @pl.when(d != me)
            def _():
                scatter(send_b, recv_b, sb_s, sb_r, d).start()
                scatter(send_m, recv_m, sm_s, sm_r, d).start()

        return 0

    lax.fori_loop(0, KH, attend, 0)

    def view_b(s):
        return all_b.at[:, pl.ds(mult(s * CB, HD), CB)]

    def reduce_b():
        recv_b[me] = send_b[me]
        recv_m[me] = send_m[me]
        scatter_wait_recv(send_m, recv_m, sm_s, sm_r)
        top = lax.fori_loop(1, n, lambda s, acc: jnp.maximum(acc, recv_m[s]), recv_m[0])
        scatter_wait_recv(send_b, recv_b, sb_s, sb_r)

        def join(s, state):
            total, mixed = state
            m = recv_m[s]
            scale = jnp.exp(m - top)
            total = total + pltpu.roll(m, HD // 2, 1) * scale
            x = recv_b[s].astype(F32)
            mixed = tuple(
                mixed[j] + x[:, j * HD : (j + 1) * HD] * scale[:, j : j + 1] for j in range(HB)
            )
            return total, mixed

        zero = jnp.zeros((S, HD), F32)
        total, mixed = lax.fori_loop(0, n, join, (zero, (zero,) * HB))
        for j in range(HB):
            h = me * HB + j
            g = h // per_group
            q = all_a[:, pl.ds(mult(h * HD, HD), HD)].astype(F32)
            key = all_a[:, pl.ds(mult(QC + g * HD, HD), HD)].astype(F32)
            val = all_a[:, pl.ds(mult(QC + KC + g * HD, HD), HD)].astype(F32)
            own = jnp.sum(q * key, axis=1, keepdims=True) * factor
            old = top[:, j : j + 1]
            best = jnp.maximum(old, own)
            old_scale = jnp.exp(old - best)
            own_weight = jnp.exp(own - best)
            bottom = total[:, j : j + 1] * old_scale + own_weight
            res = (mixed[j] * old_scale + own_weight * val) / bottom
            all_b[:, pl.ds(mult(h * HD, HD), HD)] = res.astype(BF)
        gather_start(view_b, gb_s, gb_r)

    when(owner, reduce_b)
    gather_wait_recv(view_b, gb_s, gb_r)

    NB = min(256, Dl)
    later[2].wait()

    def output_tile(j, _):
        cols = pl.ds(mult(j * NB, NB), NB)
        part_1[t, :, cols] = jnp.dot(all_b[...], wo[:, cols], preferred_element_type=F32)
        return 0

    lax.fori_loop(0, Dl // NB, output_tile, 0)
    residual = hidden[...].astype(F32) + pair_sum(part_1, t1_s, t1_r)
    sq_post = squares_block(residual)
    rg = (residual * gain_post[...]).astype(BF)
    later[3].wait()
    later[4].wait()

    def widen(k, _):
        d = lax.rem(me + 1 + k, A)
        begin = (d * FT // A) * HD
        for i, w in enumerate((wg, wu)):
            for j in range(0, W, 256):
                step = min(256, W - j)
                x = jnp.dot(
                    rg, w[:, pl.ds(mult(begin + j, HD), step)], preferred_element_type=F32
                )
                send_c[d, :, i * W + j : i * W + j + step] = x.astype(BF)
        send_c[d, :, 2 * W :] = sq_post

        @pl.when(d != me)
        def _():
            scatter(send_c, recv_c, sc_s, sc_r, d).start()

        return 0

    lax.fori_loop(0, A, widen, 0)

    def view_c(s):
        return all_c.at[s]

    def reduce_c():
        recv_c[me] = send_c[me]
        scatter_wait_recv(send_c, recv_c, sc_s, sc_r)
        total = lax.fori_loop(
            1, n, lambda s, acc: acc + recv_c[s].astype(F32), recv_c[0].astype(F32)
        )
        scale = row_scale(total[:, 2 * W :])
        gate = total[:, :W] * scale
        up = total[:, W : 2 * W] * scale
        inner = gate * jax.nn.sigmoid(gate) * up
        owned = ((me + 1) * FT // A - me * FT // A) * HD
        col = lax.broadcasted_iota(jnp.int32, (S, W), 1)
        all_c[me] = jnp.where(col < owned, inner, 0.0).astype(BF)
        gather_start(view_c, gc_s, gc_r)

    when(owner, reduce_c)
    for x in down:
        x.wait()
    gather_wait_recv(view_c, gc_s, gc_r)

    def down_tile(j, _):
        acc = jnp.zeros((S, NB), F32)
        for d in range(A):
            if d < reuse:
                w = wqkv[:, pl.ds(mult(d * Dl + j * NB, HD), NB)]
            else:
                w = tail[d - reuse, :, pl.ds(mult(j * NB, NB), NB)]
            acc = acc + jnp.dot(all_c[d], w, preferred_element_type=F32)
        part_2[t, :, pl.ds(mult(j * NB, NB), NB)] = acc
        return 0

    lax.fori_loop(0, Dl // NB, down_tile, 0)
    out[...] = (residual + pair_sum(part_2, t2_s, t2_r)).astype(BF)

    scatter_wait_send(send_a, recv_a, sa_s, sa_r)
    gather_wait_send(view_a, ga_s, ga_r)
    scatter_wait_send(send_b, recv_b, sb_s, sb_r)
    scatter_wait_send(send_m, recv_m, sm_s, sm_r)
    gather_wait_send(view_b, gb_s, gb_r)
    scatter_wait_send(send_c, recv_c, sc_s, sc_r)
    gather_wait_send(view_c, gc_s, gc_r)
    for part, s_sem, r_sem in ((part_1, t1_s, t1_r), (part_2, t2_s, t2_r)):
        for x in pair_copies(part, s_sem, r_sem):
            x.wait_send()


def per_device(
    n,
    T,
    hidden,
    lengths,
    key_cache,
    value_cache,
    gain_in,
    w_query,
    w_key,
    w_value,
    w_output,
    gain_post,
    w_gate,
    w_up,
    w_down,
):
    S, Dl = hidden.shape
    L = key_cache.shape[1]
    QC, KC = w_query.shape[1], w_key.shape[1]
    QH, KH = QC // HD, KC // HD
    FT = w_gate.shape[1] // HD
    A = max(
        a
        for a in range(1, n + 1)
        if n % a == 0
        and (QH + 2 * KH) % a == 0
        and QH % a == 0
        and (QH // KH) % (QH // a) == 0
        and a <= FT
    )
    W = -(-FT // A) * HD
    TOT = QC + 2 * KC
    reuse = min(A, TOT // Dl) if Dl == W else 0
    c = dict(n=n, T=T, A=A, S=S, Dl=Dl, L=L, QH=QH, KH=KH, W=W, FT=FT, reuse=reuse)
    CA, CB = TOT // A, QC // A
    CC = 2 * W + HD
    half = np.arange(HD) % (HD // 2)
    freq = jnp.asarray((rope_base ** (-half * 2.0 / HD)).astype(np.float32)[None, :])
    dma = pltpu.SemaphoreType.DMA
    V = pltpu.VMEM
    anywhere = pl.BlockSpec(memory_space=pl.ANY)
    vmem = pl.BlockSpec(memory_space=pltpu.VMEM)
    smem = pl.BlockSpec(memory_space=pltpu.SMEM)
    return pl.pallas_call(
        functools.partial(layer_kernel, c),
        out_shape=(
            jax.ShapeDtypeStruct((S, Dl), BF),
            jax.ShapeDtypeStruct((S, KC), BF),
            jax.ShapeDtypeStruct((S, KC), BF),
        ),
        in_specs=[smem] + [vmem] * 4 + [anywhere] * 9,
        out_specs=(vmem,) * 3,
        scratch_shapes=[
            V((Dl, TOT), BF),
            V((max(A - reuse, 1), W, Dl), BF),
            V((QC, Dl), BF),
            V((Dl, FT * HD), BF),
            V((Dl, FT * HD), BF),
            V(key_cache.shape, BF),
            V(value_cache.shape, BF),
            V((A, S, CA + HD), BF),
            V((n, S, CA + HD), BF),
            V((S, TOT), BF),
            V((A, S, CB), BF),
            V((n, S, CB), BF),
            V((A, S, HD), F32),
            V((n, S, HD), F32),
            V((S, QC), BF),
            V((T, S, Dl), F32),
            V((A, S, CC), BF),
            V((n, S, CC), BF),
            V((A, S, W), BF),
            V((T, S, Dl), F32),
            dma((8,)),
            dma((A,)),
            dma((A,)),
            dma((n,)),
            dma((n,)),
            dma((A,)),
            dma((A,)),
            dma((n,)),
            dma((A,)),
            dma((n,)),
            dma((n,)),
            dma((A,)),
            dma((T,)),
            dma((T,)),
            dma((A,)),
            dma((n,)),
            dma((n,)),
            dma((A,)),
            dma((T,)),
            dma((T,)),
        ],
        compiler_params=pltpu.CompilerParams(
            collective_id=0, has_side_effects=True, vmem_limit_bytes=67000000
        ),
    )(
        lengths,
        hidden,
        gain_in[None, :],
        gain_post[None, :],
        freq,
        key_cache,
        value_cache,
        w_query,
        w_key,
        w_value,
        w_output,
        w_gate,
        w_up,
        w_down,
    )


def solution(mesh):
    placed = (
        P("groups", "kvseq"),
        P("groups"),
        P("groups", "kvseq", "tensor"),
        P("groups", "kvseq", "tensor"),
        P("kvseq"),
        P("kvseq", "tensor"),
        P("kvseq", "tensor"),
        P("kvseq", "tensor"),
        P("tensor", "kvseq"),
        P("kvseq"),
        P("kvseq", "tensor"),
        P("kvseq", "tensor"),
        P("tensor", "kvseq"),
    )
    return jax.shard_map(
        functools.partial(per_device, mesh.shape["kvseq"], mesh.shape["tensor"]),
        mesh=mesh,
        in_specs=placed,
        out_specs=(P("groups", "kvseq"), P("groups", "tensor"), P("groups", "tensor")),
        check_vma=False,
    )
```

```python
import functools

import jax
import jax.numpy as jnp
import numpy as np
from jax import lax
from jax.experimental import pallas as pl
from jax.experimental.pallas import tpu as pltpu
from jax.sharding import PartitionSpec as P

HD = 128
epsilon = 1e-06
rope_base = 1000000.0
BF = jnp.bfloat16
F32 = jnp.float32
MESH = pl.DeviceIdType.MESH


def mult(x, m):
    return pl.multiple_of(x, m)


def when(cond, f):
    if cond is True:
        f()
    else:
        pl.when(cond)(f)


def split_kernel(packed, out, new_keys, new_values):
    Dl, KC = out.shape[1], new_keys.shape[1]
    out[...] = packed[:, :Dl]
    new_keys[...] = packed[:, Dl : Dl + KC]
    new_values[...] = packed[:, Dl + KC :]


def layer_kernel(
    c,
    lengths_hbm,
    hidden_hbm,
    gain_in_hbm,
    gain_post_hbm,
    freq_hbm,
    kc_hbm,
    vc_hbm,
    wq_hbm,
    wk_hbm,
    wv_hbm,
    wo_hbm,
    wg_hbm,
    wu_hbm,
    wd_hbm,
    out,
    lengths,
    hidden,
    gain_in,
    gain_post,
    freq,
    wqkv,
    tail,
    wo,
    wg,
    wu,
    kc,
    vc,
    early_a,
    send_a,
    recv_a,
    all_a,
    send_b,
    recv_b,
    send_m,
    recv_m,
    all_b,
    part_1,
    send_c,
    recv_c,
    all_c,
    part_2,
    wsem,
    fsem,
    dsem,
    sa_s,
    sa_r,
    ga_s,
    ga_r,
    sb_s,
    sb_r,
    sm_s,
    sm_r,
    gb_s,
    gb_r,
    t1_s,
    t1_r,
    sc_s,
    sc_r,
    gc_s,
    gc_r,
    t2_s,
    t2_r,
):
    n, T, A = c["n"], c["T"], c["A"]
    S, Dl, L = c["S"], c["Dl"], c["L"]
    QH, KH, W = c["QH"], c["KH"], c["W"]
    QC, KC = QH * HD, KH * HD
    TOT = QC + 2 * KC
    CA = TOT // A
    HA = CA // HD
    HB = QH // A
    CB = HB * HD
    FT = c["FT"]
    reuse = c["reuse"]
    per_group = QH // KH
    D = float(Dl * n)
    me = lax.axis_index("kvseq")
    t = lax.axis_index("tensor")
    owner = True if n == A else me < A

    def local(src, dst, sem):
        return pltpu.make_async_copy(src, dst, sem)

    half = Dl // 2
    first = [
        local(
            src.at[pl.ds(b * half, half), :],
            wqkv.at[pl.ds(b * half, half), pl.ds(at, width)],
            fsem.at[b * 3 + i],
        )
        for b in range(2)
        for i, (src, at, width) in enumerate(
            ((wq_hbm, 0, QC), (wk_hbm, QC, KC), (wv_hbm, QC + KC, KC))
        )
    ]
    later = [
        local(kc_hbm, kc, wsem.at[3]),
        local(vc_hbm, vc, wsem.at[4]),
        local(wo_hbm, wo, wsem.at[5]),
        local(wg_hbm, wg, wsem.at[6]),
        local(wu_hbm, wu, wsem.at[7]),
    ]

    def down_slot(d):
        return wqkv.at[:, pl.ds(d * Dl, Dl)] if d < reuse else tail.at[d - reuse]

    down = [
        local(wd_hbm.at[pl.ds((d * FT // A) * HD, W), :], down_slot(d), dsem.at[d])
        for d in range(A)
    ]
    small = [
        local(lengths_hbm, lengths, wsem.at[8]),
        local(hidden_hbm, hidden, wsem.at[9]),
        local(gain_in_hbm, gain_in, wsem.at[10]),
        local(gain_post_hbm, gain_post, wsem.at[11]),
        local(freq_hbm, freq, wsem.at[12]),
    ]
    for x in small + first:
        x.start()

    barrier = pltpu.get_barrier_semaphore()

    def greet(k, _):
        pl.semaphore_signal(
            barrier, inc=1, device_id={"kvseq": lax.rem(me + k, n)}, device_id_type=MESH
        )
        return 0

    lax.fori_loop(1, n, greet, 0)
    for k in range(1, T):
        pl.semaphore_signal(
            barrier, inc=1, device_id={"tensor": lax.rem(t + k, T)}, device_id_type=MESH
        )

    def remote(src, dst, s_sem, r_sem, to):
        return pltpu.make_async_remote_copy(
            src_ref=src, dst_ref=dst, send_sem=s_sem, recv_sem=r_sem, device_id=to,
            device_id_type=MESH,
        )

    def scatter(send, recv, s_sem, r_sem, d):
        return remote(send.at[d], recv.at[me], s_sem.at[d], r_sem.at[me], {"kvseq": d})

    def scatter_wait_recv(send, recv, s_sem, r_sem):
        def one(k, _):
            src = lax.rem(me + k, n)
            remote(
                send.at[0], recv.at[src], s_sem.at[0], r_sem.at[src], {"kvseq": src}
            ).wait_recv()
            return 0

        lax.fori_loop(1, n, one, 0)

    def scatter_wait_send(send, recv, s_sem, r_sem):
        for d in range(A):
            pl.when(d != me)(lambda d=d: scatter(send, recv, s_sem, r_sem, d).wait_send())

    def gather_start(view, s_sem, r_sem):
        def one(k, _):
            to = lax.rem(me + k, n)
            remote(view(me), view(me), s_sem.at[k], r_sem.at[me], {"kvseq": to}).start()
            return 0

        lax.fori_loop(1, n, one, 0)

    def gather_one(view, s_sem, r_sem, s):
        remote(view(s), view(s), s_sem.at[0], r_sem.at[s], {"kvseq": s}).wait_recv()

    def gather_wait_recv(view, s_sem, r_sem):
        def one(s, _):
            @pl.when(s != me)
            def _():
                remote(view(s), view(s), s_sem.at[0], r_sem.at[s], {"kvseq": s}).wait_recv()

            return 0

        lax.fori_loop(0, A, one, 0)

    def gather_wait_send(view, s_sem, r_sem):
        def one(k, _):
            to = lax.rem(me + k, n)
            remote(view(me), view(me), s_sem.at[k], r_sem.at[me], {"kvseq": to}).wait_send()
            return 0

        def run():
            lax.fori_loop(1, n, one, 0)

        when(owner, run)

    def pair_copies(part, s_sem, r_sem):
        return [
            remote(
                part.at[t], part.at[t], s_sem.at[k], r_sem.at[t], {"tensor": lax.rem(t + k, T)}
            )
            for k in range(1, T)
        ]

    def pair_sum(part, s_sem, r_sem):
        for x in pair_copies(part, s_sem, r_sem):
            x.start()
        for k in range(1, T):
            src = lax.rem(t + k, T)
            remote(
                part.at[src], part.at[src], s_sem.at[k], r_sem.at[src], {"tensor": src}
            ).wait_recv()
        total = part[0]
        for i in range(1, T):
            total = total + part[i]
        return total

    lane = lax.broadcasted_iota(jnp.int32, (S, HD), 1)
    row = lax.broadcasted_iota(jnp.int32, (S, HD), 0)

    def squares_block(x):
        s = jnp.broadcast_to(jnp.sum(x * x, axis=1, keepdims=True), (S, HD))
        high = s.astype(BF).astype(F32)
        return jnp.where(lane < HD // 2, high, s - high).astype(BF)

    def row_scale(block):
        total = jnp.sum(block, axis=1, keepdims=True) * (2.0 / HD)
        return lax.rsqrt(total / D + epsilon)

    def far_first(k):
        return lax.rem(me + A // 2 + ((k + 1) // 2) * (1 - 2 * (k % 2)) + A, A)

    def near_first(k):
        return far_first(A - 1 - k)

    for x in small:
        x.wait()
    stream = hidden[...].astype(F32)
    xg = (stream * gain_in[...]).astype(BF)
    sq = squares_block(stream)

    position = jnp.zeros((S, HD), F32)
    for s in range(S):
        position = jnp.where(row == s, lengths[s].astype(F32), position)
    angle = position * freq[...]
    cosine = jnp.cos(angle)
    sine = jnp.sin(angle)
    sine = jnp.where(lane < HD // 2, -sine, sine)

    for x in first[:3]:
        x.wait()
    def project_early(d, _):
        cols = pl.ds(mult(d * CA, HD), CA)
        early_a[d] = jnp.dot(xg[:, :half], wqkv[:half, cols], preferred_element_type=F32)
        return 0

    lax.fori_loop(0, A, project_early, 0)
    for x in first[3:]:
        x.wait()
    for x in later + down[reuse:]:
        x.start()
    pl.semaphore_wait(barrier, (n - 1) + (T - 1))

    def project(k, _):
        d = far_first(k)
        cols = pl.ds(mult(d * CA, HD), CA)
        part = early_a[d] + jnp.dot(
            xg[:, half:], wqkv[half:, cols], preferred_element_type=F32
        )
        send_a[d, :, :CA] = part.astype(BF)
        send_a[d, :, CA:] = sq

        @pl.when(d != me)
        def _():
            scatter(send_a, recv_a, sa_s, sa_r, d).start()

        return 0

    lax.fori_loop(0, A, project, 0)
    for x in down[:reuse]:
        x.start()

    def view_a(s):
        return all_a.at[:, pl.ds(mult(s * CA, HD), CA)]

    def reduce_a():
        recv_a[me] = send_a[me]
        scatter_wait_recv(send_a, recv_a, sa_s, sa_r)
        total = lax.fori_loop(
            1, n, lambda s, acc: acc + recv_a[s].astype(F32), recv_a[0].astype(F32)
        )
        scale = row_scale(total[:, CA:])
        for j in range(HA):
            v = total[:, j * HD : (j + 1) * HD] * scale
            turned = v * cosine + pltpu.roll(v, HD // 2, 1) * sine
            rot = jnp.broadcast_to(me * HA + j, (S, HD)) < QH + KH
            res = jnp.where(rot, turned, v).astype(BF)
            all_a[:, pl.ds(mult((me * HA + j) * HD, HD), HD)] = res
        gather_start(view_a, ga_s, ga_r)

    when(owner, reduce_a)
    gather_wait_recv(view_a, ga_s, ga_r)
    out[:, Dl:] = all_a[:, QC:]

    R = per_group * S
    brow = lax.broadcasted_iota(jnp.int32, (R, L), 0) % S
    orow = lax.broadcasted_iota(jnp.int32, (R, HD), 0) % S
    limit = jnp.zeros((R, L), jnp.int32)
    for s in range(S):
        limit = jnp.where(brow == s, lengths[s], limit)
    place = lax.broadcasted_iota(jnp.int32, (R, L), 1) + me * L
    valid = place < limit
    factor = float(HD) ** (-0.5)
    later[0].wait()
    later[1].wait()

    def attend(g, _):
        q = jnp.concatenate(
            [
                all_a[:, pl.ds(mult((g * per_group + j) * HD, HD), HD)].astype(F32)
                for j in range(per_group)
            ],
            axis=0,
        ).astype(BF)
        scores = jnp.zeros((R, L), F32)
        for s in range(S):
            keys = kc[s, :, pl.ds(mult(g * HD, HD), HD)]
            x = lax.dot_general(
                q, keys, (((1,), (1,)), ((), ())), preferred_element_type=F32
            )
            scores = jnp.where(brow == s, x, scores)
        scores = jnp.where(valid, scores * factor, -1e30)
        top = jnp.max(scores, axis=1, keepdims=True)
        w = jnp.where(valid, jnp.exp(scores - top), 0.0)
        total = jnp.sum(w, axis=1, keepdims=True)
        w = w.astype(BF)
        mixed = jnp.zeros((R, HD), F32)
        for s in range(S):
            vals = vc[s, :, pl.ds(mult(g * HD, HD), HD)]
            x = jnp.dot(w, vals, preferred_element_type=F32)
            mixed = jnp.where(orow == s, x, mixed)
        for i in range(per_group // HB):
            d = g * (per_group // HB) + i
            ml = jnp.zeros((S, HD), F32)
            for j in range(HB):
                r = (i * HB + j) * S
                send_b[d, :, j * HD : (j + 1) * HD] = mixed[r : r + S].astype(BF)
                ml = jnp.where(lane == j, top[r : r + S], ml)
                ml = jnp.where(lane == HD // 2 + j, total[r : r + S], ml)
            send_m[d] = ml

            @pl.when(d != me)
            def _():
                scatter(send_b, recv_b, sb_s, sb_r, d).start()
                scatter(send_m, recv_m, sm_s, sm_r, d).start()

        return 0

    lax.fori_loop(0, KH, attend, 0)

    def view_b(s):
        return all_b.at[:, pl.ds(mult(s * CB, HD), CB)]

    def reduce_b():
        recv_b[me] = send_b[me]
        recv_m[me] = send_m[me]
        scatter_wait_recv(send_m, recv_m, sm_s, sm_r)
        top = lax.fori_loop(1, n, lambda s, acc: jnp.maximum(acc, recv_m[s]), recv_m[0])
        scatter_wait_recv(send_b, recv_b, sb_s, sb_r)

        def join(s, state):
            total, mixed = state
            m = recv_m[s]
            scale = jnp.exp(m - top)
            total = total + pltpu.roll(m, HD // 2, 1) * scale
            x = recv_b[s].astype(F32)
            mixed = tuple(
                mixed[j] + x[:, j * HD : (j + 1) * HD] * scale[:, j : j + 1] for j in range(HB)
            )
            return total, mixed

        zero = jnp.zeros((S, HD), F32)
        total, mixed = lax.fori_loop(0, n, join, (zero, (zero,) * HB))
        for j in range(HB):
            h = me * HB + j
            g = h // per_group
            q = all_a[:, pl.ds(mult(h * HD, HD), HD)].astype(F32)
            key = all_a[:, pl.ds(mult(QC + g * HD, HD), HD)].astype(F32)
            val = all_a[:, pl.ds(mult(QC + KC + g * HD, HD), HD)].astype(F32)
            own = jnp.sum(q * key, axis=1, keepdims=True) * factor
            old = top[:, j : j + 1]
            best = jnp.maximum(old, own)
            old_scale = jnp.exp(old - best)
            own_weight = jnp.exp(own - best)
            bottom = total[:, j : j + 1] * old_scale + own_weight
            res = (mixed[j] * old_scale + own_weight * val) / bottom
            all_b[:, pl.ds(mult(h * HD, HD), HD)] = res.astype(BF)
        gather_start(view_b, gb_s, gb_r)

    when(owner, reduce_b)
    later[2].wait()
    part_1[t] = jnp.zeros((S, Dl), F32)

    def output_block(k, _):
        d = near_first(k)

        @pl.when(d != me)
        def _():
            gather_one(view_b, gb_s, gb_r, d)

        x = all_b[:, pl.ds(mult(d * CB, HD), CB)]
        part_1[t] += jnp.dot(x, wo[pl.ds(mult(d * CB, HD), CB), :], preferred_element_type=F32)
        return 0

    lax.fori_loop(0, A, output_block, 0)
    residual = hidden[...].astype(F32) + pair_sum(part_1, t1_s, t1_r)
    sq_post = squares_block(residual)
    rg = (residual * gain_post[...]).astype(BF)
    later[3].wait()
    later[4].wait()

    def widen(k, _):
        d = far_first(k)
        begin = (d * FT // A) * HD
        for i, w in enumerate((wg, wu)):
            for j in range(0, W, 256):
                step = min(256, W - j)
                x = jnp.dot(
                    rg, w[:, pl.ds(mult(begin + j, HD), step)], preferred_element_type=F32
                )
                send_c[d, :, i * W + j : i * W + j + step] = x.astype(BF)
        send_c[d, :, 2 * W :] = sq_post

        @pl.when(d != me)
        def _():
            scatter(send_c, recv_c, sc_s, sc_r, d).start()

        return 0

    lax.fori_loop(0, A, widen, 0)

    def view_c(s):
        return all_c.at[s]

    def reduce_c():
        recv_c[me] = send_c[me]
        scatter_wait_recv(send_c, recv_c, sc_s, sc_r)
        total = lax.fori_loop(
            1, n, lambda s, acc: acc + recv_c[s].astype(F32), recv_c[0].astype(F32)
        )
        scale = row_scale(total[:, 2 * W :])
        gate = total[:, :W] * scale
        up = total[:, W : 2 * W] * scale
        inner = gate * jax.nn.sigmoid(gate) * up
        owned = ((me + 1) * FT // A - me * FT // A) * HD
        col = lax.broadcasted_iota(jnp.int32, (S, W), 1)
        all_c[me] = jnp.where(col < owned, inner, 0.0).astype(BF)
        gather_start(view_c, gc_s, gc_r)

    when(owner, reduce_c)
    for x in down:
        x.wait()
    part_2[t] = jnp.zeros((S, Dl), F32)

    def down_block(k, _):
        d = near_first(k)

        @pl.when(d != me)
        def _():
            gather_one(view_c, gc_s, gc_r, d)

        x = all_c[d]
        if reuse:

            @pl.when(d < reuse)
            def _():
                w = wqkv[:, pl.ds(mult(d * Dl, HD), Dl)]
                part_2[t] += jnp.dot(x, w, preferred_element_type=F32)

        if reuse < A:

            @pl.when(d >= reuse)
            def _():
                w = tail[jnp.maximum(d - reuse, 0)]
                part_2[t] += jnp.dot(x, w, preferred_element_type=F32)

        return 0

    lax.fori_loop(0, A, down_block, 0)
    out[:, :Dl] = (residual + pair_sum(part_2, t2_s, t2_r)).astype(BF)

    scatter_wait_send(send_a, recv_a, sa_s, sa_r)
    gather_wait_send(view_a, ga_s, ga_r)
    scatter_wait_send(send_b, recv_b, sb_s, sb_r)
    scatter_wait_send(send_m, recv_m, sm_s, sm_r)
    gather_wait_send(view_b, gb_s, gb_r)
    scatter_wait_send(send_c, recv_c, sc_s, sc_r)
    gather_wait_send(view_c, gc_s, gc_r)
    for part, s_sem, r_sem in ((part_1, t1_s, t1_r), (part_2, t2_s, t2_r)):
        for x in pair_copies(part, s_sem, r_sem):
            x.wait_send()


def per_device(
    n,
    T,
    hidden,
    lengths,
    key_cache,
    value_cache,
    gain_in,
    w_query,
    w_key,
    w_value,
    w_output,
    gain_post,
    w_gate,
    w_up,
    w_down,
):
    S, Dl = hidden.shape
    L = key_cache.shape[1]
    QC, KC = w_query.shape[1], w_key.shape[1]
    QH, KH = QC // HD, KC // HD
    FT = w_gate.shape[1] // HD
    A = max(
        a
        for a in range(1, n + 1)
        if n % a == 0
        and (QH + 2 * KH) % a == 0
        and QH % a == 0
        and (QH // KH) % (QH // a) == 0
        and a <= FT
    )
    W = -(-FT // A) * HD
    TOT = QC + 2 * KC
    reuse = min(A, TOT // Dl) if Dl == W else 0
    c = dict(n=n, T=T, A=A, S=S, Dl=Dl, L=L, QH=QH, KH=KH, W=W, FT=FT, reuse=reuse)
    CA, CB = TOT // A, QC // A
    CC = 2 * W + HD
    half = np.arange(HD) % (HD // 2)
    freq = jnp.asarray((rope_base ** (-half * 2.0 / HD)).astype(np.float32)[None, :])
    dma = pltpu.SemaphoreType.DMA
    V = pltpu.VMEM
    anywhere = pl.BlockSpec(memory_space=pl.ANY)
    vmem = pl.BlockSpec(memory_space=pltpu.VMEM)
    packed = pl.pallas_call(
        functools.partial(layer_kernel, c),
        out_shape=jax.ShapeDtypeStruct((S, Dl + 2 * KC), BF),
        in_specs=[anywhere] * 14,
        out_specs=vmem,
        scratch_shapes=[
            pltpu.SMEM(lengths.shape, jnp.int32),
            V((S, Dl), BF),
            V((1, Dl), F32),
            V((1, Dl), F32),
            V((1, HD), F32),
            V((Dl, TOT), BF),
            V((max(A - reuse, 1), W, Dl), BF),
            V((QC, Dl), BF),
            V((Dl, FT * HD), BF),
            V((Dl, FT * HD), BF),
            V(key_cache.shape, BF),
            V(value_cache.shape, BF),
            V((A, S, CA), F32),
            V((A, S, CA + HD), BF),
            V((n, S, CA + HD), BF),
            V((S, TOT), BF),
            V((A, S, CB), BF),
            V((n, S, CB), BF),
            V((A, S, HD), F32),
            V((n, S, HD), F32),
            V((S, QC), BF),
            V((T, S, Dl), F32),
            V((A, S, CC), BF),
            V((n, S, CC), BF),
            V((A, S, W), BF),
            V((T, S, Dl), F32),
            dma((13,)),
            dma((6,)),
            dma((A,)),
            dma((A,)),
            dma((n,)),
            dma((n,)),
            dma((A,)),
            dma((A,)),
            dma((n,)),
            dma((A,)),
            dma((n,)),
            dma((n,)),
            dma((A,)),
            dma((T,)),
            dma((T,)),
            dma((A,)),
            dma((n,)),
            dma((n,)),
            dma((A,)),
            dma((T,)),
            dma((T,)),
        ],
        compiler_params=pltpu.CompilerParams(
            collective_id=0, has_side_effects=True, vmem_limit_bytes=67000000
        ),
    )(
        lengths,
        hidden,
        gain_in[None, :],
        gain_post[None, :],
        freq,
        key_cache,
        value_cache,
        w_query,
        w_key,
        w_value,
        w_output,
        w_gate,
        w_up,
        w_down,
    )
    return pl.pallas_call(
        split_kernel,
        out_shape=(
            jax.ShapeDtypeStruct((S, Dl), BF),
            jax.ShapeDtypeStruct((S, KC), BF),
            jax.ShapeDtypeStruct((S, KC), BF),
        ),
        in_specs=[vmem],
        out_specs=(vmem,) * 3,
    )(packed)


def solution(mesh):
    placed = (
        P("groups", "kvseq"),
        P("groups"),
        P("groups", "kvseq", "tensor"),
        P("groups", "kvseq", "tensor"),
        P("kvseq"),
        P("kvseq", "tensor"),
        P("kvseq", "tensor"),
        P("kvseq", "tensor"),
        P("tensor", "kvseq"),
        P("kvseq"),
        P("kvseq", "tensor"),
        P("kvseq", "tensor"),
        P("tensor", "kvseq"),
    )
    return jax.shard_map(
        functools.partial(per_device, mesh.shape["kvseq"], mesh.shape["tensor"]),
        mesh=mesh,
        in_specs=placed,
        out_specs=(P("groups", "kvseq"), P("groups", "tensor"), P("groups", "tensor")),
        check_vma=False,
    )
```

```python
import functools

import jax
import jax.numpy as jnp
import numpy as np
from jax import lax
from jax.experimental import pallas as pl
from jax.experimental.pallas import tpu as pltpu
from jax.sharding import PartitionSpec as P

HD = 128
epsilon = 1e-06
rope_base = 1000000.0
BF = jnp.bfloat16
F32 = jnp.float32
MESH = pl.DeviceIdType.MESH


def mult(x, m):
    return pl.multiple_of(x, m)


def when(cond, f):
    if cond is True:
        f()
    else:
        pl.when(cond)(f)


def split_kernel(packed, out, new_keys, new_values):
    Dl, KC = out.shape[1], new_keys.shape[1]
    out[...] = packed[:, :Dl]
    new_keys[...] = packed[:, Dl : Dl + KC]
    new_values[...] = packed[:, Dl + KC :]


def layer_kernel(
    c,
    lengths_hbm,
    hidden_hbm,
    gain_in_hbm,
    gain_post_hbm,
    freq_hbm,
    kc_hbm,
    vc_hbm,
    wq_hbm,
    wk_hbm,
    wv_hbm,
    wo_hbm,
    wg_hbm,
    wu_hbm,
    wd_hbm,
    out,
    lengths,
    hidden,
    gain_in,
    gain_post,
    freq,
    wqkv,
    tail,
    wo,
    wg,
    wu,
    kc,
    vc,
    early_a,
    send_a,
    recv_a,
    all_a,
    send_b,
    recv_b,
    send_m,
    recv_m,
    all_b,
    acc_1,
    part_1,
    send_c,
    recv_c,
    all_c,
    acc_2,
    part_2,
    wsem,
    fsem,
    dsem,
    sa_s,
    sa_r,
    ga_s,
    ga_r,
    sb_s,
    sb_r,
    sm_s,
    sm_r,
    gb_s,
    gb_r,
    t1_s,
    t1_r,
    sc_s,
    sc_r,
    gc_s,
    gc_r,
    t2_s,
    t2_r,
):
    n, T, A = c["n"], c["T"], c["A"]
    S, Dl, L = c["S"], c["Dl"], c["L"]
    QH, KH, W = c["QH"], c["KH"], c["W"]
    QC, KC = QH * HD, KH * HD
    TOT = QC + 2 * KC
    CA = TOT // A
    HA = CA // HD
    HB = QH // A
    CB = HB * HD
    FT = c["FT"]
    reuse = c["reuse"]
    per_group = QH // KH
    D = float(Dl * n)
    me = lax.axis_index("kvseq")
    t = lax.axis_index("tensor")
    owner = True if n == A else me < A

    def local(src, dst, sem):
        return pltpu.make_async_copy(src, dst, sem)

    half = Dl // 2
    first = [
        local(
            src.at[pl.ds(b * half, half), :],
            wqkv.at[pl.ds(b * half, half), pl.ds(at, width)],
            fsem.at[b * 3 + i],
        )
        for b in range(2)
        for i, (src, at, width) in enumerate(
            ((wq_hbm, 0, QC), (wk_hbm, QC, KC), (wv_hbm, QC + KC, KC))
        )
    ]
    later = [
        local(kc_hbm, kc, wsem.at[3]),
        local(vc_hbm, vc, wsem.at[4]),
        local(wo_hbm, wo, wsem.at[5]),
        local(wg_hbm, wg, wsem.at[6]),
        local(wu_hbm, wu, wsem.at[7]),
    ]

    def down_slot(d):
        return wqkv.at[:, pl.ds(d * Dl, Dl)] if d < reuse else tail.at[d - reuse]

    down = [
        local(wd_hbm.at[pl.ds((d * FT // A) * HD, W), :], down_slot(d), dsem.at[d])
        for d in range(A)
    ]
    small = [
        local(lengths_hbm, lengths, wsem.at[8]),
        local(hidden_hbm, hidden, wsem.at[9]),
        local(gain_in_hbm, gain_in, wsem.at[10]),
        local(gain_post_hbm, gain_post, wsem.at[11]),
        local(freq_hbm, freq, wsem.at[12]),
    ]
    for x in small + first:
        x.start()

    barrier = pltpu.get_barrier_semaphore()

    def greet(k, _):
        pl.semaphore_signal(
            barrier, inc=1, device_id={"kvseq": lax.rem(me + k, n)}, device_id_type=MESH
        )
        return 0

    lax.fori_loop(1, n, greet, 0)
    for k in range(1, T):
        pl.semaphore_signal(
            barrier, inc=1, device_id={"tensor": lax.rem(t + k, T)}, device_id_type=MESH
        )

    def remote(src, dst, s_sem, r_sem, to):
        return pltpu.make_async_remote_copy(
            src_ref=src, dst_ref=dst, send_sem=s_sem, recv_sem=r_sem, device_id=to,
            device_id_type=MESH,
        )

    def scatter(send, recv, s_sem, r_sem, d):
        return remote(send.at[d], recv.at[me], s_sem.at[d], r_sem.at[me], {"kvseq": d})

    def scatter_wait_recv(send, recv, s_sem, r_sem):
        def one(k, _):
            src = lax.rem(me + k, n)
            remote(
                send.at[0], recv.at[src], s_sem.at[0], r_sem.at[src], {"kvseq": src}
            ).wait_recv()
            return 0

        lax.fori_loop(1, n, one, 0)

    def scatter_wait_send(send, recv, s_sem, r_sem):
        for d in range(A):
            pl.when(d != me)(lambda d=d: scatter(send, recv, s_sem, r_sem, d).wait_send())

    def gather_to(k):
        if n % 2:
            return lax.rem(me + k, n)
        return lax.rem(me + n // 2 + (k // 2) * (1 - 2 * ((k + 1) % 2)) + n, n)

    def gather_start(view, s_sem, r_sem):
        def one(k, _):
            to = gather_to(k)
            remote(view(me), view(me), s_sem.at[k], r_sem.at[me], {"kvseq": to}).start()
            return 0

        lax.fori_loop(1, n, one, 0)

    def gather_one(view, s_sem, r_sem, s):
        remote(view(s), view(s), s_sem.at[0], r_sem.at[s], {"kvseq": s}).wait_recv()

    def gather_wait_recv(view, s_sem, r_sem):
        def one(s, _):
            @pl.when(s != me)
            def _():
                remote(view(s), view(s), s_sem.at[0], r_sem.at[s], {"kvseq": s}).wait_recv()

            return 0

        lax.fori_loop(0, A, one, 0)

    def gather_wait_send(view, s_sem, r_sem):
        def one(k, _):
            to = gather_to(k)
            remote(view(me), view(me), s_sem.at[k], r_sem.at[me], {"kvseq": to}).wait_send()
            return 0

        def run():
            lax.fori_loop(1, n, one, 0)

        when(owner, run)

    def pair_copies(part, s_sem, r_sem):
        return [
            remote(
                part.at[t], part.at[t], s_sem.at[k], r_sem.at[t], {"tensor": lax.rem(t + k, T)}
            )
            for k in range(1, T)
        ]

    def pair_sum(acc, part, s_sem, r_sem):
        part[t] = acc[...].astype(BF)
        for x in pair_copies(part, s_sem, r_sem):
            x.start()
        for k in range(1, T):
            src = lax.rem(t + k, T)
            remote(
                part.at[src], part.at[src], s_sem.at[k], r_sem.at[src], {"tensor": src}
            ).wait_recv()
        total = part[0].astype(F32)
        for i in range(1, T):
            total = total + part[i].astype(F32)
        return total

    lane = lax.broadcasted_iota(jnp.int32, (S, HD), 1)
    row = lax.broadcasted_iota(jnp.int32, (S, HD), 0)

    def squares_block(x):
        s = jnp.broadcast_to(jnp.sum(x * x, axis=1, keepdims=True), (S, HD))
        high = s.astype(BF).astype(F32)
        return jnp.where(lane < HD // 2, high, s - high).astype(BF)

    def row_scale(block):
        total = jnp.sum(block, axis=1, keepdims=True) * (2.0 / HD)
        return lax.rsqrt(total / D + epsilon)

    def far_first(k):
        return lax.rem(me + A // 2 + ((k + 1) // 2) * (1 - 2 * (k % 2)) + A, A)

    def near_first(k):
        return far_first(A - 1 - k)

    for x in small:
        x.wait()
    stream = hidden[...].astype(F32)
    xg = (stream * gain_in[...]).astype(BF)
    sq = squares_block(stream)

    position = jnp.zeros((S, HD), F32)
    for s in range(S):
        position = jnp.where(row == s, lengths[s].astype(F32), position)
    angle = position * freq[...]
    cosine = jnp.cos(angle)
    sine = jnp.sin(angle)
    sine = jnp.where(lane < HD // 2, -sine, sine)

    for x in first[:3]:
        x.wait()
    def project_early(d, _):
        cols = pl.ds(mult(d * CA, HD), CA)
        early_a[d] = jnp.dot(xg[:, :half], wqkv[:half, cols], preferred_element_type=F32)
        return 0

    lax.fori_loop(0, A, project_early, 0)
    for x in first[3:]:
        x.wait()
    for x in later + down[reuse:]:
        x.start()
    pl.semaphore_wait(barrier, (n - 1) + (T - 1))

    def project(k, _):
        d = far_first(k)
        cols = pl.ds(mult(d * CA, HD), CA)
        part = early_a[d] + jnp.dot(
            xg[:, half:], wqkv[half:, cols], preferred_element_type=F32
        )
        send_a[d, :, :CA] = part.astype(BF)
        send_a[d, :, CA:] = sq

        @pl.when(d != me)
        def _():
            scatter(send_a, recv_a, sa_s, sa_r, d).start()

        return 0

    lax.fori_loop(0, A, project, 0)
    for x in down[:reuse]:
        x.start()

    def view_a(s):
        return all_a.at[:, pl.ds(mult(s * CA, HD), CA)]

    def reduce_a():
        recv_a[me] = send_a[me]
        scatter_wait_recv(send_a, recv_a, sa_s, sa_r)
        total = lax.fori_loop(
            1, n, lambda s, acc: acc + recv_a[s].astype(F32), recv_a[0].astype(F32)
        )
        scale = row_scale(total[:, CA:])
        for j in range(HA):
            v = total[:, j * HD : (j + 1) * HD] * scale
            turned = v * cosine + pltpu.roll(v, HD // 2, 1) * sine
            rot = jnp.broadcast_to(me * HA + j, (S, HD)) < QH + KH
            res = jnp.where(rot, turned, v).astype(BF)
            all_a[:, pl.ds(mult((me * HA + j) * HD, HD), HD)] = res
        gather_start(view_a, ga_s, ga_r)

    when(owner, reduce_a)
    gather_wait_recv(view_a, ga_s, ga_r)
    out[:, Dl:] = all_a[:, QC:]

    R = per_group * S
    brow = lax.broadcasted_iota(jnp.int32, (R, L), 0) % S
    orow = lax.broadcasted_iota(jnp.int32, (R, HD), 0) % S
    limit = jnp.zeros((R, L), jnp.int32)
    for s in range(S):
        limit = jnp.where(brow == s, lengths[s], limit)
    place = lax.broadcasted_iota(jnp.int32, (R, L), 1) + me * L
    valid = place < limit
    factor = float(HD) ** (-0.5)
    later[0].wait()
    later[1].wait()

    def attend(g, _):
        q = jnp.concatenate(
            [
                all_a[:, pl.ds(mult((g * per_group + j) * HD, HD), HD)].astype(F32)
                for j in range(per_group)
            ],
            axis=0,
        ).astype(BF)
        scores = jnp.zeros((R, L), F32)
        for s in range(S):
            keys = kc[s, :, pl.ds(mult(g * HD, HD), HD)]
            x = lax.dot_general(
                q, keys, (((1,), (1,)), ((), ())), preferred_element_type=F32
            )
            scores = jnp.where(brow == s, x, scores)
        scores = jnp.where(valid, scores * factor, -1e30)
        top = jnp.max(scores, axis=1, keepdims=True)
        w = jnp.where(valid, jnp.exp(scores - top), 0.0)
        total = jnp.sum(w, axis=1, keepdims=True)
        w = w.astype(BF)
        mixed = jnp.zeros((R, HD), F32)
        for s in range(S):
            vals = vc[s, :, pl.ds(mult(g * HD, HD), HD)]
            x = jnp.dot(w, vals, preferred_element_type=F32)
            mixed = jnp.where(orow == s, x, mixed)
        for i in range(per_group // HB):
            d = g * (per_group // HB) + i
            ml = jnp.zeros((S, HD), F32)
            for j in range(HB):
                r = (i * HB + j) * S
                send_b[d, :, j * HD : (j + 1) * HD] = mixed[r : r + S].astype(BF)
                ml = jnp.where(lane == j, top[r : r + S], ml)
                ml = jnp.where(lane == HD // 2 + j, total[r : r + S], ml)
            send_m[d] = ml

            @pl.when(d != me)
            def _():
                scatter(send_b, recv_b, sb_s, sb_r, d).start()
                scatter(send_m, recv_m, sm_s, sm_r, d).start()

        return 0

    lax.fori_loop(0, KH, attend, 0)

    def view_b(s):
        return all_b.at[:, pl.ds(mult(s * CB, HD), CB)]

    def reduce_b():
        recv_b[me] = send_b[me]
        recv_m[me] = send_m[me]
        scatter_wait_recv(send_m, recv_m, sm_s, sm_r)
        top = lax.fori_loop(1, n, lambda s, acc: jnp.maximum(acc, recv_m[s]), recv_m[0])
        scatter_wait_recv(send_b, recv_b, sb_s, sb_r)

        def join(s, state):
            total, mixed = state
            m = recv_m[s]
            scale = jnp.exp(m - top)
            total = total + pltpu.roll(m, HD // 2, 1) * scale
            x = recv_b[s].astype(F32)
            mixed = tuple(
                mixed[j] + x[:, j * HD : (j + 1) * HD] * scale[:, j : j + 1] for j in range(HB)
            )
            return total, mixed

        zero = jnp.zeros((S, HD), F32)
        total, mixed = lax.fori_loop(0, n, join, (zero, (zero,) * HB))
        for j in range(HB):
            h = me * HB + j
            g = h // per_group
            q = all_a[:, pl.ds(mult(h * HD, HD), HD)].astype(F32)
            key = all_a[:, pl.ds(mult(QC + g * HD, HD), HD)].astype(F32)
            val = all_a[:, pl.ds(mult(QC + KC + g * HD, HD), HD)].astype(F32)
            own = jnp.sum(q * key, axis=1, keepdims=True) * factor
            old = top[:, j : j + 1]
            best = jnp.maximum(old, own)
            old_scale = jnp.exp(old - best)
            own_weight = jnp.exp(own - best)
            bottom = total[:, j : j + 1] * old_scale + own_weight
            res = (mixed[j] * old_scale + own_weight * val) / bottom
            all_b[:, pl.ds(mult(h * HD, HD), HD)] = res.astype(BF)
        gather_start(view_b, gb_s, gb_r)

    when(owner, reduce_b)
    later[2].wait()
    acc_1[...] = jnp.zeros((S, Dl), F32)

    def output_block(k, _):
        d = near_first(k)

        @pl.when(d != me)
        def _():
            gather_one(view_b, gb_s, gb_r, d)

        x = all_b[:, pl.ds(mult(d * CB, HD), CB)]
        acc_1[...] += jnp.dot(x, wo[pl.ds(mult(d * CB, HD), CB), :], preferred_element_type=F32)
        return 0

    lax.fori_loop(0, A, output_block, 0)
    residual = hidden[...].astype(F32) + pair_sum(acc_1, part_1, t1_s, t1_r)
    sq_post = squares_block(residual)
    rg = (residual * gain_post[...]).astype(BF)
    later[3].wait()
    later[4].wait()

    def widen(k, _):
        d = far_first(k)
        begin = (d * FT // A) * HD
        for i, w in enumerate((wg, wu)):
            for j in range(0, W, 256):
                step = min(256, W - j)
                x = jnp.dot(
                    rg, w[:, pl.ds(mult(begin + j, HD), step)], preferred_element_type=F32
                )
                send_c[d, :, i * W + j : i * W + j + step] = x.astype(BF)
        send_c[d, :, 2 * W :] = sq_post

        @pl.when(d != me)
        def _():
            scatter(send_c, recv_c, sc_s, sc_r, d).start()

        return 0

    lax.fori_loop(0, A, widen, 0)

    def view_c(s):
        return all_c.at[s]

    def reduce_c():
        recv_c[me] = send_c[me]
        scatter_wait_recv(send_c, recv_c, sc_s, sc_r)
        total = lax.fori_loop(
            1, n, lambda s, acc: acc + recv_c[s].astype(F32), recv_c[0].astype(F32)
        )
        scale = row_scale(total[:, 2 * W :])
        gate = total[:, :W] * scale
        up = total[:, W : 2 * W] * scale
        inner = gate * jax.nn.sigmoid(gate) * up
        owned = ((me + 1) * FT // A - me * FT // A) * HD
        col = lax.broadcasted_iota(jnp.int32, (S, W), 1)
        all_c[me] = jnp.where(col < owned, inner, 0.0).astype(BF)
        gather_start(view_c, gc_s, gc_r)

    when(owner, reduce_c)
    for x in down:
        x.wait()
    acc_2[...] = jnp.zeros((S, Dl), F32)

    def down_block(k, _):
        d = near_first(k)

        @pl.when(d != me)
        def _():
            gather_one(view_c, gc_s, gc_r, d)

        x = all_c[d]
        if reuse:

            @pl.when(d < reuse)
            def _():
                w = wqkv[:, pl.ds(mult(d * Dl, HD), Dl)]
                acc_2[...] += jnp.dot(x, w, preferred_element_type=F32)

        if reuse < A:

            @pl.when(d >= reuse)
            def _():
                w = tail[jnp.maximum(d - reuse, 0)]
                acc_2[...] += jnp.dot(x, w, preferred_element_type=F32)

        return 0

    lax.fori_loop(0, A, down_block, 0)
    out[:, :Dl] = (residual + pair_sum(acc_2, part_2, t2_s, t2_r)).astype(BF)

    scatter_wait_send(send_a, recv_a, sa_s, sa_r)
    gather_wait_send(view_a, ga_s, ga_r)
    scatter_wait_send(send_b, recv_b, sb_s, sb_r)
    scatter_wait_send(send_m, recv_m, sm_s, sm_r)
    gather_wait_send(view_b, gb_s, gb_r)
    scatter_wait_send(send_c, recv_c, sc_s, sc_r)
    gather_wait_send(view_c, gc_s, gc_r)
    for part, s_sem, r_sem in ((part_1, t1_s, t1_r), (part_2, t2_s, t2_r)):
        for x in pair_copies(part, s_sem, r_sem):
            x.wait_send()


def per_device(
    n,
    T,
    hidden,
    lengths,
    key_cache,
    value_cache,
    gain_in,
    w_query,
    w_key,
    w_value,
    w_output,
    gain_post,
    w_gate,
    w_up,
    w_down,
):
    S, Dl = hidden.shape
    L = key_cache.shape[1]
    QC, KC = w_query.shape[1], w_key.shape[1]
    QH, KH = QC // HD, KC // HD
    FT = w_gate.shape[1] // HD
    A = max(
        a
        for a in range(1, n + 1)
        if n % a == 0
        and (QH + 2 * KH) % a == 0
        and QH % a == 0
        and (QH // KH) % (QH // a) == 0
        and a <= FT
    )
    W = -(-FT // A) * HD
    TOT = QC + 2 * KC
    reuse = min(A, TOT // Dl) if Dl == W else 0
    c = dict(n=n, T=T, A=A, S=S, Dl=Dl, L=L, QH=QH, KH=KH, W=W, FT=FT, reuse=reuse)
    CA, CB = TOT // A, QC // A
    CC = 2 * W + HD
    half = np.arange(HD) % (HD // 2)
    freq = jnp.asarray((rope_base ** (-half * 2.0 / HD)).astype(np.float32)[None, :])
    dma = pltpu.SemaphoreType.DMA
    V = pltpu.VMEM
    anywhere = pl.BlockSpec(memory_space=pl.ANY)
    vmem = pl.BlockSpec(memory_space=pltpu.VMEM)
    packed = pl.pallas_call(
        functools.partial(layer_kernel, c),
        out_shape=jax.ShapeDtypeStruct((S, Dl + 2 * KC), BF),
        in_specs=[anywhere] * 14,
        out_specs=vmem,
        scratch_shapes=[
            pltpu.SMEM(lengths.shape, jnp.int32),
            V((S, Dl), BF),
            V((1, Dl), F32),
            V((1, Dl), F32),
            V((1, HD), F32),
            V((Dl, TOT), BF),
            V((max(A - reuse, 1), W, Dl), BF),
            V((QC, Dl), BF),
            V((Dl, FT * HD), BF),
            V((Dl, FT * HD), BF),
            V(key_cache.shape, BF),
            V(value_cache.shape, BF),
            V((A, S, CA), F32),
            V((A, S, CA + HD), BF),
            V((n, S, CA + HD), BF),
            V((S, TOT), BF),
            V((A, S, CB), BF),
            V((n, S, CB), BF),
            V((A, S, HD), F32),
            V((n, S, HD), F32),
            V((S, QC), BF),
            V((S, Dl), F32),
            V((T, S, Dl), BF),
            V((A, S, CC), BF),
            V((n, S, CC), BF),
            V((A, S, W), BF),
            V((S, Dl), F32),
            V((T, S, Dl), BF),
            dma((13,)),
            dma((6,)),
            dma((A,)),
            dma((A,)),
            dma((n,)),
            dma((n,)),
            dma((A,)),
            dma((A,)),
            dma((n,)),
            dma((A,)),
            dma((n,)),
            dma((n,)),
            dma((A,)),
            dma((T,)),
            dma((T,)),
            dma((A,)),
            dma((n,)),
            dma((n,)),
            dma((A,)),
            dma((T,)),
            dma((T,)),
        ],
        compiler_params=pltpu.CompilerParams(
            collective_id=0, has_side_effects=True, vmem_limit_bytes=67000000
        ),
    )(
        lengths,
        hidden,
        gain_in[None, :],
        gain_post[None, :],
        freq,
        key_cache,
        value_cache,
        w_query,
        w_key,
        w_value,
        w_output,
        w_gate,
        w_up,
        w_down,
    )
    return pl.pallas_call(
        split_kernel,
        out_shape=(
            jax.ShapeDtypeStruct((S, Dl), BF),
            jax.ShapeDtypeStruct((S, KC), BF),
            jax.ShapeDtypeStruct((S, KC), BF),
        ),
        in_specs=[vmem],
        out_specs=(vmem,) * 3,
    )(packed)


def solution(mesh):
    placed = (
        P("groups", "kvseq"),
        P("groups"),
        P("groups", "kvseq", "tensor"),
        P("groups", "kvseq", "tensor"),
        P("kvseq"),
        P("kvseq", "tensor"),
        P("kvseq", "tensor"),
        P("kvseq", "tensor"),
        P("tensor", "kvseq"),
        P("kvseq"),
        P("kvseq", "tensor"),
        P("kvseq", "tensor"),
        P("tensor", "kvseq"),
    )
    return jax.shard_map(
        functools.partial(per_device, mesh.shape["kvseq"], mesh.shape["tensor"]),
        mesh=mesh,
        in_specs=placed,
        out_specs=(P("groups", "kvseq"), P("groups", "tensor"), P("groups", "tensor")),
        check_vma=False,
    )
```
